128 devices in a mesh: groups: 4 (over x, y), wide: 32 (over z, core).
Axes of the slice: x: 2, y: 2, z: 16, core: 2. Of those that a mesh axis runs over, the one named last changes fastest.
The devices are a block of a 8x8x16 slice.
Arguments:
- half_integrals: float32 [1024, 512, 800], P(('groups', 'wide')), parts along dimension 0, may hold values from -40 to 40
- pair_list: int32 [1024, 2], P('groups'), parts along dimension 0, may hold values from 0 to 199, as said below
- occupied_energy: float32 [800], P('groups'), parts along dimension 0, may hold values from -3 to -0.3
- virtual_orbitals: float32 [3200, 600], P('groups'), parts along dimension 0, may hold values from -0.21875 to 0.21875
- tile_order: int32 [64], replicated, may hold values from 0 to 63, each once
Outputs:
- transformed: float32 [1024, 512, 600], P('groups', 'wide'), parts along dimension 0
- pair_rms: float32 [1024], P('groups'), parts along dimension 0
The draws below stay inside these ranges and needn't reach their ends.
There are 4 independent parts, one for each index of `groups`. The reference program is written for one: setup_inputs(seed, part) draws one part's arguments, and reference() takes and returns one part's arrays. A program takes and returns all parts, laid end to end along the dimension named above; an argument that names none is the same for every part. Nothing has to cross between parts.
Inputs may be any that keep to these rules, and one draw needn't show every extreme that they name: `pair_list`: each row is a distinct pair (i, j) with i <= j.
All inputs are finite; a program needn't handle non-finite values.
Results may differ from the reference program's by a relative error of at most 0.00007.
Values sent between devices are 32-bit elements; how exact they have to be, the bound alone decides.
No kernel may reach another device: no remote copies, remote signals or barrier semaphores. Data moves between devices by JAX's collectives and lax.ppermute only.
A program may use at most 128 MiB of HBM per device.

```python
import jax
import jax.numpy as jnp
from jax import lax

NOCC = 200
NBAS = 800
NVIRT = 600
S_WIN = 512
TILE_S = 8
PAIRS = 256
TILES = 64


def draw_half_integrals(key, part):
    scale_key = jax.random.fold_in(key, 11)
    base_key = jax.random.fold_in(key, 12)
    column_scale = jnp.exp(jax.random.uniform(scale_key, (S_WIN,), jnp.float32, jnp.log(0.3), jnp.log(3.0)))
    base = jnp.clip(jax.random.normal(base_key, (PAIRS, S_WIN, NBAS), jnp.float32), -6.0, 6.0)
    return (base * column_scale[None, :, None]).astype(jnp.float32)


def draw_pair_list(key, part):
    total = NOCC * (NOCC + 1) // 2
    chosen = jax.random.permutation(jax.random.fold_in(key, 21), total)[:PAIRS].astype(jnp.int32)
    orbital = jnp.arange(NOCC, dtype=jnp.int32)
    triangle = orbital * (orbital + 1) // 2
    second = jnp.sum((triangle[None, :] <= chosen[:, None]).astype(jnp.int32), axis=1) - 1
    first = chosen - jnp.take(triangle, second)
    return jnp.stack([first, second], axis=1).astype(jnp.int32)


def normal_values(own_key, shape, width, most, kind=jnp.bfloat16):
    values = jax.random.normal(own_key, shape, jnp.float32) * width
    return jnp.minimum(jnp.maximum(values, -most), most).astype(kind)


def setup_inputs(seed: int = 0, part: int = 0) -> dict:
    keys = jax.random.split(jax.random.key(seed), 6)
    part_keys = jax.random.split(jax.random.fold_in(keys[5], part), 6)
    return {
        "half_integrals": draw_half_integrals(jax.random.fold_in(jax.random.fold_in(keys[5], part), 71), part),
        "pair_list": draw_pair_list(jax.random.fold_in(jax.random.fold_in(keys[5], part), 71), part),
        "occupied_energy": jnp.clip(jax.random.uniform(part_keys[2], (NOCC,), jnp.float32, -3.0, -0.3), -3.0, -0.3),
        "virtual_orbitals": normal_values(part_keys[3], (NBAS, NVIRT), NBAS ** -0.5, 0.21875, jnp.float32),
        "tile_order": jax.random.permutation(keys[4], TILES).astype(jnp.int32),
    }


def reference(half_integrals, pair_list, occupied_energy, virtual_orbitals, tile_order):
    energy_sum = occupied_energy[pair_list[:, 0]] + occupied_energy[pair_list[:, 1]]
    weights = jnp.exp(0.3 * energy_sum).astype(jnp.float32)
    pair_count = half_integrals.shape[0]
    tiled = half_integrals.reshape(pair_count, TILES, TILE_S, NBAS)
    ordered = jnp.take(tiled, tile_order, axis=1).reshape(pair_count, S_WIN, NBAS)
    product = jnp.einsum('psr,ra->psa', ordered, virtual_orbitals, precision=lax.Precision.HIGHEST)
    transformed = product * weights[:, None, None]
    squares = lax.optimization_barrier(jnp.sum(transformed * transformed, axis=(1, 2)))
    pair_rms = jnp.sqrt(squares / (S_WIN * NVIRT) + 1e-06)
    return (transformed, pair_rms)
```

```python
import functools

import jax
import jax.numpy as jnp
from jax import lax
from jax.experimental import pallas as pl
from jax.experimental.pallas import tpu as pltpu
from jax.sharding import PartitionSpec as P

TILE_S = 8
LANES = 128
ROWS = 16
CHUNKS = 5
UNPACK_ROWS = 40


def pair_weights(pair_list, occupied_energy):
    orbital = jnp.arange(occupied_energy.shape[0], dtype=jnp.int32)
    first = jnp.sum(
        jnp.where(pair_list[:, 0:1] == orbital[None, :], occupied_energy[None, :], 0.0), axis=1
    )
    second = jnp.sum(
        jnp.where(pair_list[:, 1:2] == orbital[None, :], occupied_energy[None, :], 0.0), axis=1
    )
    return jnp.exp(0.3 * (first + second))


def split(x):
    high = x.astype(jnp.bfloat16)
    return high, (x - high.astype(jnp.float32)).astype(jnp.bfloat16)


def blocks_kernel(shifts, peers, pos, order, half, orbitals, *refs):
    outs, squares = refs[: len(shifts)], refs[len(shifts)]
    data, high, low, sems = refs[len(shifts) + 1 :]
    pairs, basis, _ = data.shape
    span = basis // CHUNKS
    copies = [
        pltpu.make_async_copy(
            half.at[:, pl.ds(c * span, span), :], data.at[:, pl.ds(c * span, span), :], sems.at[c]
        )
        for c in range(CHUNKS)
    ]
    for copy in copies:
        copy.start()
    lane = lax.broadcasted_iota(jnp.int32, (ROWS, LANES), 1)
    inner = (lane // pairs) % TILE_S
    first = lane < LANES // 2
    member = lane % pairs
    where_from = []
    for shift in shifts:
        owner = lax.rem(pos[0] + shift, peers)
        tiles = [order[2 * owner], order[2 * owner + 1]]
        per_block = LANES // TILE_S
        starts = [pl.multiple_of((t // per_block) * LANES, LANES) for t in tiles]
        index = [inner + (t % per_block) * TILE_S for t in tiles]
        where_from.append((starts, index))

    def gather(step, carry):
        rows = pl.ds(pl.multiple_of(step * ROWS, ROWS), ROWS)
        for n, (starts, index) in enumerate(where_from):
            block = None
            for p in range(pairs):
                a, b = (
                    jnp.take_along_axis(
                        data[p, rows, pl.ds(s, LANES)], i, axis=1, mode="promise_in_bounds"
                    )
                    for s, i in zip(starts, index)
                )
                both = jnp.where(first, a, b)
                block = both if block is None else jnp.where(member == p, both, block)
            columns = pl.ds(n * LANES, LANES)
            high[rows, columns], low[rows, columns] = split(block)
        return carry

    for c in range(CHUNKS):
        copies[c].wait()
        lax.fori_loop(c * span // ROWS, (c + 1) * span // ROWS, gather, 0)
    v_high, v_low = split(orbitals[...])
    total = None
    dot = functools.partial(jnp.dot, preferred_element_type=jnp.float32)
    for n in range(0, len(shifts), 2):
        width = min(2, len(shifts) - n)
        columns = pl.ds(n * LANES, width * LANES)
        h, l = high[:, columns], low[:, columns]
        product = dot(v_high, l) + dot(v_low, h) + dot(v_high, h)
        for m in range(width):
            block = product[:, m * LANES : (m + 1) * LANES]
            outs[n + m][...] = block
            part = jnp.sum((block * block).reshape(-1, 8, LANES), axis=0)
            total = part if total is None else total + part
    squares[...] = total


def blocks_for(shifts, peers, pos, order, half, orbitals):
    pairs, basis, columns = half.shape
    virtuals = orbitals.shape[0]
    n = len(shifts)
    smem = pl.BlockSpec(memory_space=pltpu.SMEM)
    vmem = pl.BlockSpec(memory_space=pltpu.VMEM)
    results = pl.pallas_call(
        functools.partial(blocks_kernel, shifts, peers),
        in_specs=[smem, smem, pl.BlockSpec(memory_space=pl.ANY), vmem],
        out_specs=[vmem] * (n + 1),
        out_shape=[jax.ShapeDtypeStruct((virtuals, LANES), jnp.float32)] * n
        + [jax.ShapeDtypeStruct((8, LANES), jnp.float32)],
        scratch_shapes=[
            pltpu.VMEM((pairs, basis, columns), jnp.float32),
            pltpu.VMEM((basis, n * LANES), jnp.bfloat16),
            pltpu.VMEM((basis, n * LANES), jnp.bfloat16),
            pltpu.SemaphoreType.DMA((CHUNKS,)),
        ],
        cost_estimate=pl.CostEstimate(
            flops=6 * n * LANES * basis * virtuals,
            bytes_accessed=4 * pairs * basis * columns,
            transcendentals=0,
        ),
        name=f"blocks_{shifts[0]}",
    )(pos, order, half, orbitals)
    return results[:n], results[n]


def unpack_kernel(peers, pairs, pos, weights, *refs):
    ins, out = refs[:peers], refs[peers]
    per = LANES // pairs
    lane = lax.broadcasted_iota(jnp.int32, (8, LANES), 1)
    group = lane // pairs
    shift = pos[0] * pairs
    inner = lax.rem(shift, LANES)
    outer = lax.div(shift, LANES)
    wrapped = lane < inner
    count = peers // per

    def tile(step, carry):
        rows = pl.ds(pl.multiple_of(step * 8, 8), 8)
        halves = []
        for b in range(count):
            x = [ins[b * per + j][rows, :] for j in range(per)]
            m = 1
            while m < per:
                upper = (group & m) != 0
                y = list(x)
                for i in range(per):
                    if not i & m:
                        j = i | m
                        y[i] = jnp.where(upper, pltpu.roll(x[j], pairs * m, 1), x[i])
                        y[j] = jnp.where(upper, x[j], pltpu.roll(x[i], LANES - pairs * m, 1))
                x = y
                m *= 2
            halves.append(x)
        for k in range(per):
            rolled = [pltpu.roll(halves[b][k], inner, 1) for b in range(count)]
            for b in range(count):
                place = pl.multiple_of(lax.rem(b + outer, count) * LANES, LANES)
                value = jnp.where(wrapped, rolled[b - 1], rolled[b])
                out[k, rows, pl.ds(place, LANES)] = value * weights[:, pl.ds(place, LANES)]
        return carry

    lax.fori_loop(0, out.shape[1] // 8, tile, 0)


def unpack(blocks, pos, weights, pairs):
    peers = len(blocks)
    virtuals = blocks[0].shape[0]
    per = LANES // pairs
    total = weights.shape[1]
    r = UNPACK_ROWS
    return pl.pallas_call(
        functools.partial(unpack_kernel, peers, pairs),
        grid=(virtuals // r,),
        in_specs=[
            pl.BlockSpec(memory_space=pltpu.SMEM),
            pl.BlockSpec((1, total), lambda i: (0, 0)),
        ]
        + [pl.BlockSpec((r, LANES), lambda i: (i, 0))] * peers,
        out_specs=pl.BlockSpec((per, r, total), lambda i: (0, i, 0)),
        out_shape=jax.ShapeDtypeStruct((per, virtuals, total), jnp.float32),
        name="unpack",
    )(pos, weights, *blocks)


def order_of_shifts(peers):
    far = []
    for d in range(peers // 2 - 1, 0, -1):
        far += [d, peers - d]
    far.insert(2, peers // 2)
    return far + [0]


def shards(half_integrals, pair_list, occupied_energy, virtual_orbitals, tile_order):
    pairs, columns, basis = half_integrals.shape
    virtuals = virtual_orbitals.shape[1]
    peers = lax.axis_size("wide")
    pos = lax.axis_index("wide").astype(jnp.int32).reshape(1)
    half = jnp.swapaxes(half_integrals, 1, 2)
    orbitals = virtual_orbitals.T
    shifts = order_of_shifts(peers)
    groups = [shifts[:4]] + [shifts[i : i + 4] for i in range(4, peers, 4)]
    arrived = {}
    sums = []
    for g in groups:
        blocks, part = blocks_for(tuple(g), peers, pos, tile_order, half, orbitals)
        sums.append(part)
        for s, block in zip(g, blocks):
            moved = block if s == 0 else lax.ppermute(
                block, "wide", [(i, (i + s) % peers) for i in range(peers)]
            )
            arrived[(peers - s) % peers] = moved
    squares = jnp.sum(jnp.sum(sum(sums), axis=0).reshape(LANES // pairs, pairs), axis=0)
    sent = jnp.broadcast_to(squares[None, None], (peers, 1, pairs))
    totals = lax.all_to_all(sent, "wide", 0, 0, tiled=True).reshape(peers * pairs)
    weights = pair_weights(pair_list, occupied_energy)
    pair_rms = jnp.sqrt(totals * weights * weights / (columns * virtuals) + 1e-06)
    out = unpack([arrived[i] for i in range(peers)], pos, weights[None], pairs)
    return (jnp.transpose(out, (2, 0, 1)), pair_rms)


def solution(mesh):
    in_specs = (
        P(("groups", "wide"), None, None),
        P("groups", None),
        P("groups"),
        P("groups", None),
        P(),
    )
    out_specs = (P("groups", "wide", None), P("groups"))
    return jax.shard_map(shards, mesh=mesh, in_specs=in_specs, out_specs=out_specs, check_vma=False)
```

```python
import functools

import jax
import jax.numpy as jnp
from jax import lax
from jax.experimental import pallas as pl
from jax.experimental.pallas import tpu as pltpu
from jax.sharding import PartitionSpec as P


TILE_S = 8
LANES = 128
CHUNKS = 5
GATHER_ROWS = 80
STEP = 40
PACK = 280
UNPACK = 80
LAST = 40
EARLY = (2, 2)


SMEM = pl.BlockSpec(memory_space=pltpu.SMEM)
VMEM = pl.BlockSpec(memory_space=pltpu.VMEM)
ANY = pl.BlockSpec(memory_space=pl.ANY)


def pair_weights(pair_list, occupied_energy):
    orbital = jnp.arange(occupied_energy.shape[0], dtype=jnp.int32)
    first = jnp.sum(
        jnp.where(pair_list[:, 0:1] == orbital[None, :], occupied_energy[None, :], 0.0), axis=1
    )
    second = jnp.sum(
        jnp.where(pair_list[:, 1:2] == orbital[None, :], occupied_energy[None, :], 0.0), axis=1
    )
    return jnp.exp(0.3 * (first + second))


def split(x):
    high = x.astype(jnp.bfloat16)
    return high, (x - high.astype(jnp.float32)).astype(jnp.bfloat16)


def product_of(v_high, v_low, high, low):
    dot = functools.partial(jnp.dot, preferred_element_type=jnp.float32)
    return dot(v_high, low) + dot(v_low, high) + dot(v_high, high)


def paired_order(rows, pairs):
    lane = lax.broadcasted_iota(jnp.int32, (rows, LANES), 1)
    half = pairs * TILE_S
    return (lane // half) * half + (lane % pairs) * TILE_S + (lane // pairs) % TILE_S


def take_lanes(x, index):
    return jnp.take_along_axis(x, index, axis=1, mode="promise_in_bounds")


def early_kernel(shifts, peers, first, pos, order, half, *refs):
    n = len(shifts)
    if first:
        orbitals, refs = refs[0], refs[1:]
        outs, (v_high, v_low) = refs[:n], refs[n : n + 2]
        data, high, low, sems = refs[n + 2 :]
    else:
        v_high, v_low = refs[:2]
        outs = refs[2 : n + 2]
        data, high, low, sems = refs[n + 2 :]
    pairs, basis, _ = data.shape
    rows_out = outs[0].shape[0]
    span = basis // CHUNKS
    copies = [
        pltpu.make_async_copy(
            half.at[:, pl.ds(c * span, span), :], data.at[:, pl.ds(c * span, span), :], sems.at[c]
        )
        for c in range(CHUNKS)
    ]
    for copy in copies:
        copy.start()
    if first:
        v_high[...], v_low[...] = split(orbitals[...].T)
    group = lax.broadcasted_iota(jnp.int32, (GATHER_ROWS, LANES), 1) // TILE_S
    index = paired_order(GATHER_ROWS, pairs)
    per_block = LANES // TILE_S
    sources = []
    for shift in shifts:
        owner = lax.rem(pos[0] + shift, peers)
        for h in range(2):
            tile = order[2 * owner + h]
            start = pl.multiple_of((tile // per_block) * LANES, LANES)
            sources.append((start, h * pairs, lax.rem(tile, per_block)))

    def gather(step, carry):
        rows = pl.ds(pl.multiple_of(step * GATHER_ROWS, GATHER_ROWS), GATHER_ROWS)
        for n in range(len(shifts)):
            block = None
            for start, base, place in sources[2 * n : 2 * n + 2]:
                for p in range(pairs):
                    amount = lax.rem((base + p - place + per_block) * TILE_S, LANES)
                    x = pltpu.roll(data[p, rows, pl.ds(start, LANES)], amount, 1)
                    block = x if block is None else jnp.where(group == base + p, x, block)
            columns = pl.ds(n * LANES, LANES)
            high[rows, columns], low[rows, columns] = split(take_lanes(block, index))
        return carry

    for c in range(CHUNKS):
        copies[c].wait()
        lax.fori_loop(c * span // GATHER_ROWS, (c + 1) * span // GATHER_ROWS, gather, 0)
    product = product_of(v_high[:rows_out], v_low[:rows_out], high[...], low[...])
    for m in range(n):
        outs[m][...] = product[:, m * LANES : (m + 1) * LANES]


def early_blocks(shifts, peers, cut, pos, order, half, *orbitals):
    pairs, basis, columns = half.shape
    first = len(orbitals) == 1
    virtuals = orbitals[0].shape[1 if first else 0]
    n = len(shifts)
    more = [jax.ShapeDtypeStruct((virtuals, basis), jnp.bfloat16)] * 2 if first else []
    return pl.pallas_call(
        functools.partial(early_kernel, shifts, peers, first),
        in_specs=[SMEM, SMEM, ANY] + [VMEM] * len(orbitals),
        out_specs=[VMEM] * (n + len(more)),
        out_shape=[jax.ShapeDtypeStruct((cut, LANES), jnp.float32)] * n + more,
        scratch_shapes=[
            pltpu.VMEM((pairs, basis, columns), jnp.float32),
            pltpu.VMEM((basis, n * LANES), jnp.bfloat16),
            pltpu.VMEM((basis, n * LANES), jnp.bfloat16),
            pltpu.SemaphoreType.DMA((CHUNKS,)),
        ],
        cost_estimate=pl.CostEstimate(
            flops=6 * n * LANES * basis * virtuals,
            bytes_accessed=4 * pairs * basis * columns,
            transcendentals=0,
        ),
    )(pos, order, half, *orbitals)


def rest_kernel(shifts, peers, skipped, pos, order, half, v_high, v_low, *refs):
    n = len(shifts) - skipped
    outs = refs[:n]
    ends, squares, products, tiles = refs[n:]
    pairs, virtuals, columns = products.shape
    steps = (virtuals - LAST) // PACK
    step = pl.program_id(0)
    blocks = columns // LANES
    per_block = LANES // TILE_S

    @pl.when(step < pairs)
    def _():
        high, low = split(half[0])
        product = product_of(v_high[...], v_low[...], high, low)
        products[step] = product
        sums = jnp.sum((product * product).reshape(virtuals // 8, 8, columns), axis=0)
        total = sums[:, :LANES]
        for b in range(1, blocks):
            total = total + sums[:, b * LANES : (b + 1) * LANES]
        squares[0] = total

    group = lax.broadcasted_iota(jnp.int32, (STEP, LANES), 1) // TILE_S
    index = paired_order(STEP, pairs)
    front = group < pairs

    def source(owner, h):
        tile = order[2 * owner + h]
        within = lax.rem(tile, per_block)
        place = (tile // per_block) * pairs + lax.rem(within, pairs)
        return place, lax.rem(within // pairs + h, 2) * (LANES // 2)

    def block_for(owner):
        a, turn_a = source(owner, 0)
        c, turn_c = source(owner, 1)
        return jnp.where(front, pltpu.roll(tiles[a], turn_a, 1), pltpu.roll(tiles[c], turn_c, 1))

    def fill(row):
        rows_in = pl.ds(pl.multiple_of(row, 8), STEP)

        def one(b, carry):
            columns_in = pl.ds(pl.multiple_of(b * LANES, LANES), LANES)
            x = [products[p, rows_in, columns_in] for p in range(pairs)]
            m = 1
            while m < pairs:
                upper = (group & m) != 0
                y = list(x)
                for p in range(pairs):
                    if not p & m:
                        q = p | m
                        y[p] = jnp.where(upper, pltpu.roll(x[q], TILE_S * m, 1), x[p])
                        y[q] = jnp.where(upper, x[q], pltpu.roll(x[p], LANES - TILE_S * m, 1))
                x = y
                m *= 2
            for p in range(pairs):
                tiles[b * pairs + p] = take_lanes(x[p], index)
            return carry

        lax.fori_loop(0, blocks, one, 0)

    @pl.when((step >= pairs) & (step < pairs + steps))
    def _():
        def one(i, carry):
            fill((step - pairs) * PACK + i * STEP)
            rows_out = pl.ds(pl.multiple_of(i * STEP, 8), STEP)
            for j, shift in enumerate(shifts[skipped:]):
                outs[j][rows_out, :] = block_for(lax.rem(pos[0] + shift, peers))
            return carry

        lax.fori_loop(0, PACK // STEP, one, 0)

    @pl.when(step == pairs + steps)
    def _():
        fill(virtuals - LAST)

        def one(owner, carry):
            ends[owner] = block_for(owner)
            return carry

        lax.fori_loop(0, peers, one, 0)


def rest_blocks(shifts, peers, skipped, pos, order, half, v_high, v_low):
    pairs, basis, columns = half.shape
    virtuals = v_high.shape[0]
    n = len(shifts) - skipped
    cut = virtuals - LAST
    steps = cut // PACK
    results = pl.pallas_call(
        functools.partial(rest_kernel, shifts, peers, skipped),
        grid=(pairs + steps + 1,),
        in_specs=[
            SMEM,
            SMEM,
            pl.BlockSpec((1, basis, columns), lambda i: (jnp.minimum(i, pairs - 1), 0, 0)),
        ]
        + [pl.BlockSpec((virtuals, basis), lambda i: (0, 0))] * 2,
        out_specs=[pl.BlockSpec((PACK, LANES), lambda i: (jnp.clip(i - pairs, 0, steps - 1), 0))] * n
        + [
            pl.BlockSpec((peers, LAST, LANES), lambda i: (0, 0, 0)),
            pl.BlockSpec((1, 8, LANES), lambda i: (jnp.minimum(i, pairs - 1), 0, 0)),
        ],
        out_shape=[jax.ShapeDtypeStruct((cut, LANES), jnp.float32)] * n
        + [
            jax.ShapeDtypeStruct((peers, LAST, LANES), jnp.float32),
            jax.ShapeDtypeStruct((pairs, 8, LANES), jnp.float32),
        ],
        scratch_shapes=[
            pltpu.VMEM((pairs, virtuals, columns), jnp.float32),
            pltpu.VMEM((columns * pairs // LANES, STEP, LANES), jnp.float32),
        ],
        cost_estimate=pl.CostEstimate(
            flops=6 * pairs * columns * basis * virtuals,
            bytes_accessed=4 * pairs * basis * columns,
            transcendentals=0,
        ),
        name="rest_blocks",
    )(pos, order, half, v_high, v_low)
    return results[:n], results[n], results[n + 1]


def regroup(x, pairs, upper_of):
    m = 1
    while m < len(x):
        upper = upper_of(m)
        y = list(x)
        for i in range(len(x)):
            if not i & m:
                j = i | m
                y[i] = jnp.where(upper, pltpu.roll(x[j], pairs * m, 1), x[i])
                y[j] = jnp.where(upper, x[j], pltpu.roll(x[i], LANES - pairs * m, 1))
        x = y
        m *= 2
    return x


def unpack_kernel(peers, pairs, pos, weights, *refs):
    ins, out = refs[:peers], refs[-1]
    per = LANES // pairs
    group = lax.broadcasted_iota(jnp.int32, (STEP, LANES), 1) // pairs
    shift = pos[0] * pairs
    inner = lax.rem(shift, LANES)
    outer = lax.div(shift, LANES)
    wrapped = group * pairs < inner
    count = peers // per

    def tile(step, carry):
        rows = pl.ds(pl.multiple_of(step * STEP, 8), STEP)
        halves = [
            regroup(
                [ins[b * per + j][rows, :] for j in range(per)], pairs, lambda m: (group & m) != 0
            )
            for b in range(count)
        ]
        for k in range(per):
            rolled = [pltpu.roll(halves[b][k], inner, 1) for b in range(count)]
            for b in range(count):
                place = pl.multiple_of(lax.rem(b + outer, count) * LANES, LANES)
                value = jnp.where(wrapped, rolled[b - 1], rolled[b])
                out[k, rows, pl.ds(place, LANES)] = value * weights[:, pl.ds(place, LANES)]
        return carry

    lax.fori_loop(0, out.shape[1] // STEP, tile, 0)


def unpack(blocks, pos, weights, pairs, virtuals):
    peers = len(blocks)
    per = LANES // pairs
    total = weights.shape[1]
    return pl.pallas_call(
        functools.partial(unpack_kernel, peers, pairs),
        grid=(blocks[0].shape[0] // UNPACK,),
        in_specs=[SMEM, pl.BlockSpec((1, total), lambda i: (0, 0))]
        + [pl.BlockSpec((UNPACK, LANES), lambda i: (i, 0))] * peers,
        out_specs=pl.BlockSpec((per, UNPACK, total), lambda i: (0, i, 0)),
        out_shape=jax.ShapeDtypeStruct((per, virtuals, total), jnp.float32),
        name="unpack",
    )(pos, weights, *blocks)


def unpack_last_kernel(pairs, weights, ends, _, out):
    peers, rows, _ = ends.shape
    per = LANES // pairs
    group = lax.broadcasted_iota(jnp.int32, (rows, LANES), 1) // pairs
    for b in range(peers // per):
        lanes = pl.ds(b * LANES, LANES)
        done = regroup(
            [ends[b * per + j] for j in range(per)], pairs, lambda m: (group & m) != 0
        )
        for k in range(per):
            out[k, :, lanes] = done[k] * weights[:, lanes]


def unpack_last(ends, weights, pairs, into):
    per, virtuals, total = into.shape
    rows = ends.shape[1]
    return pl.pallas_call(
        functools.partial(unpack_last_kernel, pairs),
        grid=(1,),
        in_specs=[
            pl.BlockSpec((1, total), lambda i: (0, 0)),
            pl.BlockSpec(ends.shape, lambda i: (0, 0, 0)),
            ANY,
        ],
        out_specs=pl.BlockSpec((per, rows, total), lambda i: (0, virtuals // rows - 1, 0)),
        out_shape=jax.ShapeDtypeStruct(into.shape, into.dtype),
        input_output_aliases={2: 0},
        name="unpack_last",
    )(weights, ends, into)


def order_of_shifts(peers):
    far = []
    for d in range(peers // 2 - 1, 0, -1):
        far += [d, peers - d]
    far.insert(sum(EARLY), peers // 2)
    return far + [0]


def shards(half_integrals, pair_list, occupied_energy, virtual_orbitals, tile_order):
    pairs, columns, _ = half_integrals.shape
    virtuals = virtual_orbitals.shape[1]
    peers = lax.axis_size("wide")
    cut = virtuals - LAST
    pos = lax.axis_index("wide").astype(jnp.int32).reshape(1)
    half = jnp.swapaxes(half_integrals, 1, 2)
    shifts = tuple(order_of_shifts(peers))
    blocks = []
    kept = [virtual_orbitals]
    at = 0
    for n in EARLY:
        results = early_blocks(shifts[at : at + n], peers, cut, pos, tile_order, half, *kept)
        blocks += results[:n]
        kept = results[n:] or kept
        at += n
    more, ends, sums = rest_blocks(shifts, peers, at, pos, tile_order, half, *kept)
    blocks += more
    arrived = {}
    for n, s in enumerate(shifts):
        block = blocks[n]
        if s:
            block = lax.ppermute(block, "wide", [(i, (i + s) % peers) for i in range(peers)])
        arrived[(peers - s) % peers] = block
    squares = jnp.sum(sums, axis=(1, 2))
    sent = jnp.broadcast_to(squares[None, None], (peers, 1, pairs))
    totals = lax.all_to_all(sent, "wide", 0, 0, tiled=True).reshape(peers * pairs)
    ends = lax.all_to_all(ends, "wide", 0, 0, tiled=True)
    weights = pair_weights(pair_list, occupied_energy)
    pair_rms = jnp.sqrt(totals * weights * weights / (columns * virtuals) + 1e-06)
    out = unpack([arrived[i] for i in range(peers)], pos, weights[None], pairs, virtuals)
    out = unpack_last(ends, weights[None], pairs, out)
    return (jnp.transpose(out, (2, 0, 1)), pair_rms)


def solution(mesh):
    in_specs = (
        P(("groups", "wide"), None, None),
        P("groups", None),
        P("groups"),
        P("groups", None),
        P(),
    )
    out_specs = (P("groups", "wide", None), P("groups"))
    return jax.shard_map(shards, mesh=mesh, in_specs=in_specs, out_specs=out_specs, check_vma=False)
```

```python
import functools

import jax
import jax.numpy as jnp
from jax import lax
from jax.experimental import pallas as pl
from jax.experimental.pallas import tpu as pltpu
from jax.sharding import PartitionSpec as P


TILE_S = 8
LANES = 128
CHUNKS = 5
AHEAD = 2
STEP = 40
PACK = 280
UNPACK = 80
LAST = 40
UNROLL = 2
EARLY = (1, 2, 4)


SMEM = pl.BlockSpec(memory_space=pltpu.SMEM)
VMEM = pl.BlockSpec(memory_space=pltpu.VMEM)
ANY = pl.BlockSpec(memory_space=pl.ANY)


def pair_weights(pair_list, occupied_energy):
    orbital = jnp.arange(occupied_energy.shape[0], dtype=jnp.int32)
    first = jnp.sum(
        jnp.where(pair_list[:, 0:1] == orbital[None, :], occupied_energy[None, :], 0.0), axis=1
    )
    second = jnp.sum(
        jnp.where(pair_list[:, 1:2] == orbital[None, :], occupied_energy[None, :], 0.0), axis=1
    )
    return jnp.exp(0.3 * (first + second))


def split(x):
    high = x.astype(jnp.bfloat16)
    return high, (x - high.astype(jnp.float32)).astype(jnp.bfloat16)


def product_of(v_high, v_low, high, low):
    dot = functools.partial(jnp.dot, preferred_element_type=jnp.float32)
    return dot(v_high, low) + dot(v_low, high) + dot(v_high, high)


def turned(rows, turn):
    lane = lax.broadcasted_iota(jnp.int32, (rows, LANES), 1)
    return (lane - turn + LANES) % LANES


def paired_order(lane, pairs):
    half = pairs * TILE_S
    return (lane // half) * half + (lane % pairs) * TILE_S + (lane // pairs) % TILE_S


def own_turn(pos, pairs):
    return lax.rem(pos[0] * pairs, LANES)


def take_lanes(x, index):
    return jnp.take_along_axis(x, index, axis=1, mode="promise_in_bounds")


def early_kernel(shifts, peers, first, pos, order, half, *refs):
    n = len(shifts)
    if first:
        orbitals, refs = refs[0], refs[1:]
        outs, kept = refs[:n], refs[n : n + 2]
        data, high, low, sems, v_in, v_high, v_low, v_sems = refs[n + 2 :]
    else:
        v_high, v_low = refs[:2]
        outs = refs[2 : n + 2]
        data, high, low, sems = refs[n + 2 :]
    pairs, basis, _ = data.shape
    rows_out = outs[0].shape[0]
    span = basis // CHUNKS

    def piece(c):
        rows = pl.ds(pl.multiple_of(c * span, span), span)
        return pltpu.make_async_copy(half.at[:, rows, :], data.at[:, rows, :], sems.at[c])

    if first:
        v_copy = pltpu.make_async_copy(orbitals, v_in, v_sems.at[0])
        v_copy.start()
    for c in range(AHEAD):
        piece(c).start()
    if first:
        v_copy.wait()
        v_high[...], v_low[...] = split(v_in[...].T)
        keep = [
            pltpu.make_async_copy(x, y, v_sems.at[1 + m])
            for m, (x, y) in enumerate(zip((v_high, v_low), kept))
        ]
    group = lax.broadcasted_iota(jnp.int32, (span, LANES), 1) // TILE_S
    index = paired_order(turned(span, own_turn(pos, pairs)), pairs)
    per_block = LANES // TILE_S
    sources = []
    for shift in shifts:
        owner = lax.rem(pos[0] + shift, peers)
        for h in range(2):
            tile = order[2 * owner + h]
            start = pl.multiple_of((tile // per_block) * LANES, LANES)
            sources.append((start, h * pairs, lax.rem(tile, per_block)))

    def gather(step, carry):
        piece(step).wait()

        @pl.when(step + AHEAD < CHUNKS)
        def _():
            piece(step + AHEAD).start()

        rows = pl.ds(pl.multiple_of(step * span, span), span)
        for n in range(len(shifts)):
            block = None
            for start, base, place in sources[2 * n : 2 * n + 2]:
                for p in range(pairs):
                    amount = lax.rem((base + p - place + per_block) * TILE_S, LANES)
                    x = pltpu.roll(data[p, rows, pl.ds(start, LANES)], amount, 1)
                    block = x if block is None else jnp.where(group == base + p, x, block)
            columns = pl.ds(n * LANES, LANES)
            high[rows, columns], low[rows, columns] = split(take_lanes(block, index))
        return carry

    lax.fori_loop(0, CHUNKS, gather, 0)
    if first:
        for copy in keep:
            copy.start()
    product = product_of(v_high[:rows_out], v_low[:rows_out], high[...], low[...])
    for m in range(n):
        outs[m][...] = product[:, m * LANES : (m + 1) * LANES]
    if first:
        for copy in keep:
            copy.wait()


def early_blocks(shifts, peers, cut, pos, order, half, *orbitals):
    pairs, basis, columns = half.shape
    first = len(orbitals) == 1
    virtuals = orbitals[0].shape[1 if first else 0]
    n = len(shifts)
    more = [jax.ShapeDtypeStruct((virtuals, basis), jnp.bfloat16)] * 2 if first else []
    return pl.pallas_call(
        functools.partial(early_kernel, shifts, peers, first),
        in_specs=[SMEM, SMEM, ANY] + [ANY if first else VMEM] * len(orbitals),
        out_specs=[VMEM] * n + [ANY] * len(more),
        out_shape=[jax.ShapeDtypeStruct((cut, LANES), jnp.float32)] * n + more,
        scratch_shapes=[
            pltpu.VMEM((pairs, basis, columns), jnp.float32),
            pltpu.VMEM((basis, n * LANES), jnp.bfloat16),
            pltpu.VMEM((basis, n * LANES), jnp.bfloat16),
            pltpu.SemaphoreType.DMA((CHUNKS,)),
        ]
        + (
            [
                pltpu.VMEM((basis, virtuals), jnp.float32),
                pltpu.VMEM((virtuals, basis), jnp.bfloat16),
                pltpu.VMEM((virtuals, basis), jnp.bfloat16),
                pltpu.SemaphoreType.DMA((3,)),
            ]
            if first
            else []
        ),
        cost_estimate=pl.CostEstimate(
            flops=6 * n * LANES * basis * virtuals,
            bytes_accessed=4 * pairs * basis * columns,
            transcendentals=0,
        ),
    )(pos, order, half, *orbitals)


def rest_kernel(shifts, peers, skipped, pos, order, half, v_high, v_low, *refs):
    n = len(shifts) - skipped
    outs = refs[:n]
    ends, squares, products, tiles = refs[n:]
    pairs, virtuals, columns = products.shape
    steps = (virtuals - LAST) // PACK
    step = pl.program_id(0)
    blocks = columns // LANES
    per_block = LANES // TILE_S

    @pl.when(step < pairs)
    def _():
        high, low = split(half[0])
        product = product_of(v_high[...], v_low[...], high, low)
        products[step] = product
        sums = jnp.sum((product * product).reshape(virtuals // 8, 8, columns), axis=0)
        total = sums[:, :LANES]
        for b in range(1, blocks):
            total = total + sums[:, b * LANES : (b + 1) * LANES]
        squares[0] = total

    group = lax.broadcasted_iota(jnp.int32, (STEP, LANES), 1) // TILE_S
    turn = own_turn(pos, pairs)
    index = paired_order(turned(STEP, 0), pairs)
    front = turned(STEP, turn) < LANES // 2

    def source(owner, h):
        tile = order[2 * owner + h]
        within = lax.rem(tile, per_block)
        place = (tile // per_block) * pairs + lax.rem(within, pairs)
        return place, lax.rem(lax.rem(within // pairs + h, 2) * (LANES // 2) + turn, LANES)

    def block_for(owner):
        a, turn_a = source(owner, 0)
        c, turn_c = source(owner, 1)
        return jnp.where(front, pltpu.roll(tiles[a], turn_a, 1), pltpu.roll(tiles[c], turn_c, 1))

    def fill(row):
        rows_in = pl.ds(pl.multiple_of(row, 8), STEP)

        def one(b, carry):
            columns_in = pl.ds(pl.multiple_of(b * LANES, LANES), LANES)
            x = [products[p, rows_in, columns_in] for p in range(pairs)]
            m = 1
            while m < pairs:
                upper = (group & m) != 0
                y = list(x)
                for p in range(pairs):
                    if not p & m:
                        q = p | m
                        y[p] = jnp.where(upper, pltpu.roll(x[q], TILE_S * m, 1), x[p])
                        y[q] = jnp.where(upper, x[q], pltpu.roll(x[p], LANES - TILE_S * m, 1))
                x = y
                m *= 2
            for p in range(pairs):
                tiles[b * pairs + p] = take_lanes(x[p], index)
            return carry

        lax.fori_loop(0, blocks, one, 0)

    @pl.when((step >= pairs) & (step < pairs + steps))
    def _():
        def one(i, carry):
            fill((step - pairs) * PACK + i * STEP)
            rows_out = pl.ds(pl.multiple_of(i * STEP, 8), STEP)
            for j, shift in enumerate(shifts[skipped:]):
                outs[j][rows_out, :] = block_for(lax.rem(pos[0] + shift, peers))
            return carry

        lax.fori_loop(0, PACK // STEP, one, 0)

    @pl.when(step == pairs + steps)
    def _():
        fill(virtuals - LAST)

        def one(owner, carry):
            ends[owner] = block_for(owner)
            return carry

        lax.fori_loop(0, peers, one, 0)


def rest_blocks(shifts, peers, skipped, pos, order, half, v_high, v_low):
    pairs, basis, columns = half.shape
    virtuals = v_high.shape[0]
    n = len(shifts) - skipped
    cut = virtuals - LAST
    steps = cut // PACK
    results = pl.pallas_call(
        functools.partial(rest_kernel, shifts, peers, skipped),
        grid=(pairs + steps + 1,),
        in_specs=[
            SMEM,
            SMEM,
            pl.BlockSpec((1, basis, columns), lambda i: (jnp.minimum(i, pairs - 1), 0, 0)),
        ]
        + [pl.BlockSpec((virtuals, basis), lambda i: (0, 0))] * 2,
        out_specs=[pl.BlockSpec((PACK, LANES), lambda i: (jnp.clip(i - pairs, 0, steps - 1), 0))] * n
        + [
            pl.BlockSpec((peers, LAST, LANES), lambda i: (0, 0, 0)),
            pl.BlockSpec((1, 8, LANES), lambda i: (jnp.minimum(i, pairs - 1), 0, 0)),
        ],
        out_shape=[jax.ShapeDtypeStruct((cut, LANES), jnp.float32)] * n
        + [
            jax.ShapeDtypeStruct((peers, LAST, LANES), jnp.float32),
            jax.ShapeDtypeStruct((pairs, 8, LANES), jnp.float32),
        ],
        scratch_shapes=[
            pltpu.VMEM((pairs, virtuals, columns), jnp.float32),
            pltpu.VMEM((columns * pairs // LANES, STEP, LANES), jnp.float32),
        ],
        cost_estimate=pl.CostEstimate(
            flops=6 * pairs * columns * basis * virtuals,
            bytes_accessed=4 * pairs * basis * columns,
            transcendentals=0,
        ),
        name="rest_blocks",
    )(pos, order, half, v_high, v_low)
    return results[:n], results[n], results[n + 1]


def merge(x, pairs, ahead):
    n = len(x)
    group = lax.broadcasted_iota(jnp.int32, x[0].shape, 1) // pairs
    behind = (group - ahead + n) % n
    m = 1
    while m < n:
        far = (behind & m) != 0
        x = [jnp.where(far, x[(j + m) % n], x[j]) for j in range(n)]
        m *= 2
    turns = [(LANES - k * pairs) % LANES for k in range(n)]
    return [pltpu.roll(x[-k % n], t, 1) if t else x[0] for k, t in enumerate(turns)]


def unpack_kernel(peers, pairs, pos, weights, *refs):
    ins, out = refs[:peers], refs[-1]
    per = LANES // pairs
    ahead = lax.rem(pos[0], per)
    outer = lax.div(pos[0], per)
    group = lax.broadcasted_iota(jnp.int32, (8, LANES), 1) // pairs
    straight = group >= ahead
    count = peers // per

    def one(step, carry):
        for t in range(UNROLL):
            rows = pl.ds(pl.multiple_of((step * UNROLL + t) * 8, 8), 8)
            halves = [
                merge([ins[b * per + j][rows, :] for j in range(per)], pairs, ahead)
                for b in range(count)
            ]
            for b in range(count):
                place = pl.multiple_of(lax.rem(b + outer, count) * LANES, LANES)
                scale = weights[:, pl.ds(place, LANES)]
                for k in range(per):
                    value = jnp.where(straight, halves[b][k], halves[b - 1][k])
                    out[k, rows, pl.ds(place, LANES)] = value * scale
        return carry

    lax.fori_loop(0, out.shape[1] // (8 * UNROLL), one, 0)


def unpack(blocks, pos, weights, pairs, virtuals):
    peers = len(blocks)
    per = LANES // pairs
    total = weights.shape[1]
    return pl.pallas_call(
        functools.partial(unpack_kernel, peers, pairs),
        grid=(blocks[0].shape[0] // UNPACK,),
        in_specs=[SMEM, pl.BlockSpec((1, total), lambda i: (0, 0))]
        + [pl.BlockSpec((UNPACK, LANES), lambda i: (i, 0))] * peers,
        out_specs=pl.BlockSpec((per, UNPACK, total), lambda i: (0, i, 0)),
        out_shape=jax.ShapeDtypeStruct((per, virtuals, total), jnp.float32),
        name="unpack",
    )(pos, weights, *blocks)


def unpack_last_kernel(pairs, weights, ends, _, out):
    peers, rows, _ = ends.shape
    per = LANES // pairs

    def one(step, carry):
        at = pl.ds(pl.multiple_of(step * 8, 8), 8)
        for b in range(peers // per):
            lanes = pl.ds(b * LANES, LANES)
            done = merge([ends[b * per + j, at, :] for j in range(per)], pairs, 0)
            for k in range(per):
                out[k, at, lanes] = done[k] * weights[:, lanes]
        return carry

    lax.fori_loop(0, rows // 8, one, 0, unroll=True)


def unpack_last(ends, weights, pairs, into):
    per, virtuals, total = into.shape
    rows = ends.shape[1]
    return pl.pallas_call(
        functools.partial(unpack_last_kernel, pairs),
        grid=(1,),
        in_specs=[
            pl.BlockSpec((1, total), lambda i: (0, 0)),
            pl.BlockSpec(ends.shape, lambda i: (0, 0, 0)),
            ANY,
        ],
        out_specs=pl.BlockSpec((per, rows, total), lambda i: (0, virtuals // rows - 1, 0)),
        out_shape=jax.ShapeDtypeStruct(into.shape, into.dtype),
        input_output_aliases={2: 0},
        name="unpack_last",
    )(weights, ends, into)


def order_of_shifts(peers):
    shifts = [peers // 2]
    for d in range(peers // 2 - 1, 0, -1):
        shifts += [d, peers - d]
    return shifts + [0]


def shards(half_integrals, pair_list, occupied_energy, virtual_orbitals, tile_order):
    pairs, columns, _ = half_integrals.shape
    virtuals = virtual_orbitals.shape[1]
    peers = lax.axis_size("wide")
    cut = virtuals - LAST
    pos = lax.axis_index("wide").astype(jnp.int32).reshape(1)
    half = jnp.swapaxes(half_integrals, 1, 2)
    shifts = tuple(order_of_shifts(peers))
    blocks = []
    kept = [virtual_orbitals]
    at = 0
    for n in EARLY:
        results = early_blocks(shifts[at : at + n], peers, cut, pos, tile_order, half, *kept)
        blocks += results[:n]
        kept = results[n:] or kept
        at += n
    more, ends, sums = rest_blocks(shifts, peers, at, pos, tile_order, half, *kept)
    blocks += more
    arrived = {}
    for n, s in enumerate(shifts):
        block = blocks[n]
        if s:
            block = lax.ppermute(block, "wide", [(i, (i + s) % peers) for i in range(peers)])
        arrived[(peers - s) % peers] = block
    squares = jnp.sum(sums, axis=(1, 2))
    sent = jnp.broadcast_to(squares[None, None], (peers, 1, pairs))
    totals = lax.all_to_all(sent, "wide", 0, 0, tiled=True).reshape(peers * pairs)
    ends = lax.all_to_all(ends, "wide", 0, 0, tiled=True)
    weights = pair_weights(pair_list, occupied_energy)
    pair_rms = jnp.sqrt(totals * weights * weights / (columns * virtuals) + 1e-06)
    out = unpack([arrived[i] for i in range(peers)], pos, weights[None], pairs, virtuals)
    out = unpack_last(ends, weights[None], pairs, out)
    return (jnp.transpose(out, (2, 0, 1)), pair_rms)


def solution(mesh):
    in_specs = (
        P(("groups", "wide"), None, None),
        P("groups", None),
        P("groups"),
        P("groups", None),
        P(),
    )
    out_specs = (P("groups", "wide", None), P("groups"))
    return jax.shard_map(shards, mesh=mesh, in_specs=in_specs, out_specs=out_specs, check_vma=False)
```

```python
import functools

import jax
import jax.numpy as jnp
from jax import lax
from jax.experimental import pallas as pl
from jax.experimental.pallas import tpu as pltpu
from jax.sharding import PartitionSpec as P


TILE_S = 8
LANES = 128
CHUNKS = 5
AHEAD = 3
STEP = 40
PACK = 280
UNPACK = 80
LAST = 40
UNROLL = 2
UNPACK_VMEM = 66_600_000
EARLY = (2, 2, 3)


SMEM = pl.BlockSpec(memory_space=pltpu.SMEM)
VMEM = pl.BlockSpec(memory_space=pltpu.VMEM)
ANY = pl.BlockSpec(memory_space=pl.ANY)


def pair_weights(pair_list, occupied_energy):
    orbital = jnp.arange(occupied_energy.shape[0], dtype=jnp.int32)
    first = jnp.sum(
        jnp.where(pair_list[:, 0:1] == orbital[None, :], occupied_energy[None, :], 0.0), axis=1
    )
    second = jnp.sum(
        jnp.where(pair_list[:, 1:2] == orbital[None, :], occupied_energy[None, :], 0.0), axis=1
    )
    return jnp.exp(0.3 * (first + second))


def split(x):
    high = x.astype(jnp.bfloat16)
    return high, (x - high.astype(jnp.float32)).astype(jnp.bfloat16)


def product_of(v_high, v_low, high, low):
    dot = functools.partial(jnp.dot, preferred_element_type=jnp.float32)
    return dot(v_high, low) + dot(v_low, high) + dot(v_high, high)


def turned(rows, turn):
    lane = lax.broadcasted_iota(jnp.int32, (rows, LANES), 1)
    return (lane - turn + LANES) % LANES


def paired_order(lane, pairs):
    half = pairs * TILE_S
    return (lane // half) * half + (lane % pairs) * TILE_S + (lane // pairs) % TILE_S


def own_turn(pos, pairs):
    return lax.rem(pos[0] * pairs, LANES)


def take_lanes(x, index):
    return jnp.take_along_axis(x, index, axis=1, mode="promise_in_bounds")


def early_kernel(shifts, peers, first, pos, order, half, *refs):
    n = len(shifts)
    if first:
        orbitals, refs = refs[0], refs[1:]
        outs, kept = refs[:n], refs[n : n + 2]
        data, high, low, sems, v_in, v_high, v_low, v_sems = refs[n + 2 :]
    else:
        v_high, v_low = refs[:2]
        outs = refs[2 : n + 2]
        data, high, low, sems = refs[n + 2 :]
    pairs, basis, _ = data.shape
    rows_out = outs[0].shape[0]
    span = basis // CHUNKS

    def piece(c):
        rows = pl.ds(pl.multiple_of(c * span, span), span)
        return pltpu.make_async_copy(half.at[:, rows, :], data.at[:, rows, :], sems.at[c])

    if first:
        v_copy = pltpu.make_async_copy(orbitals, v_in, v_sems.at[0])
        v_copy.start()
    for c in range(AHEAD):
        piece(c).start()
    if first:
        v_copy.wait()
        v_high[...], v_low[...] = split(v_in[...].T)
        keep = [
            pltpu.make_async_copy(x, y, v_sems.at[1 + m])
            for m, (x, y) in enumerate(zip((v_high, v_low), kept))
        ]
    group = lax.broadcasted_iota(jnp.int32, (span, LANES), 1) // TILE_S
    index = paired_order(turned(span, own_turn(pos, pairs)), pairs)
    per_block = LANES // TILE_S
    sources = []
    for shift in shifts:
        owner = lax.rem(pos[0] + shift, peers)
        for h in range(2):
            tile = order[2 * owner + h]
            start = pl.multiple_of((tile // per_block) * LANES, LANES)
            sources.append((start, h * pairs, lax.rem(tile, per_block)))

    def gather(step, carry):
        piece(step).wait()

        @pl.when(step + AHEAD < CHUNKS)
        def _():
            piece(step + AHEAD).start()

        rows = pl.ds(pl.multiple_of(step * span, span), span)
        for n in range(len(shifts)):
            block = None
            for start, base, place in sources[2 * n : 2 * n + 2]:
                for p in range(pairs):
                    amount = lax.rem((base + p - place + per_block) * TILE_S, LANES)
                    x = pltpu.roll(data[p, rows, pl.ds(start, LANES)], amount, 1)
                    block = x if block is None else jnp.where(group == base + p, x, block)
            columns = pl.ds(n * LANES, LANES)
            high[rows, columns], low[rows, columns] = split(take_lanes(block, index))
        return carry

    lax.fori_loop(0, CHUNKS, gather, 0)
    if first:
        for copy in keep:
            copy.start()
    product = product_of(v_high[:rows_out], v_low[:rows_out], high[...], low[...])
    for m in range(n):
        outs[m][...] = product[:, m * LANES : (m + 1) * LANES]
    if first:
        for copy in keep:
            copy.wait()


def early_blocks(shifts, peers, cut, pos, order, half, *orbitals):
    pairs, basis, columns = half.shape
    first = len(orbitals) == 1
    virtuals = orbitals[0].shape[1 if first else 0]
    n = len(shifts)
    more = [jax.ShapeDtypeStruct((virtuals, basis), jnp.bfloat16)] * 2 if first else []
    return pl.pallas_call(
        functools.partial(early_kernel, shifts, peers, first),
        in_specs=[SMEM, SMEM, ANY] + [ANY if first else VMEM] * len(orbitals),
        out_specs=[VMEM] * n + [ANY] * len(more),
        out_shape=[jax.ShapeDtypeStruct((cut, LANES), jnp.float32)] * n + more,
        scratch_shapes=[
            pltpu.VMEM((pairs, basis, columns), jnp.float32),
            pltpu.VMEM((basis, n * LANES), jnp.bfloat16),
            pltpu.VMEM((basis, n * LANES), jnp.bfloat16),
            pltpu.SemaphoreType.DMA((CHUNKS,)),
        ]
        + (
            [
                pltpu.VMEM((basis, virtuals), jnp.float32),
                pltpu.VMEM((virtuals, basis), jnp.bfloat16),
                pltpu.VMEM((virtuals, basis), jnp.bfloat16),
                pltpu.SemaphoreType.DMA((3,)),
            ]
            if first
            else []
        ),
        cost_estimate=pl.CostEstimate(
            flops=6 * n * LANES * basis * virtuals,
            bytes_accessed=4 * pairs * basis * columns,
            transcendentals=0,
        ),
    )(pos, order, half, *orbitals)


def rest_kernel(shifts, peers, skipped, pos, order, half, v_high, v_low, *refs):
    n = len(shifts) - skipped
    outs = refs[:n]
    ends, squares, products, tiles = refs[n:]
    pairs, virtuals, columns = products.shape
    steps = (virtuals - LAST) // PACK
    step = pl.program_id(0)
    blocks = columns // LANES
    per_block = LANES // TILE_S

    @pl.when(step < pairs)
    def _():
        high, low = split(half[0])
        product = product_of(v_high[...], v_low[...], high, low)
        products[step] = product
        sums = jnp.sum((product * product).reshape(virtuals // 8, 8, columns), axis=0)
        total = sums[:, :LANES]
        for b in range(1, blocks):
            total = total + sums[:, b * LANES : (b + 1) * LANES]
        squares[0] = total

    group = lax.broadcasted_iota(jnp.int32, (STEP, LANES), 1) // TILE_S
    turn = own_turn(pos, pairs)
    index = paired_order(turned(STEP, 0), pairs)
    front = turned(STEP, turn) < LANES // 2

    def source(owner, h):
        tile = order[2 * owner + h]
        within = lax.rem(tile, per_block)
        place = (tile // per_block) * pairs + lax.rem(within, pairs)
        return place, lax.rem(lax.rem(within // pairs + h, 2) * (LANES // 2) + turn, LANES)

    def block_for(owner):
        a, turn_a = source(owner, 0)
        c, turn_c = source(owner, 1)
        return jnp.where(front, pltpu.roll(tiles[a], turn_a, 1), pltpu.roll(tiles[c], turn_c, 1))

    def fill(row):
        rows_in = pl.ds(pl.multiple_of(row, 8), STEP)

        def one(b, carry):
            columns_in = pl.ds(pl.multiple_of(b * LANES, LANES), LANES)
            x = [products[p, rows_in, columns_in] for p in range(pairs)]
            m = 1
            while m < pairs:
                upper = (group & m) != 0
                y = list(x)
                for p in range(pairs):
                    if not p & m:
                        q = p | m
                        y[p] = jnp.where(upper, pltpu.roll(x[q], TILE_S * m, 1), x[p])
                        y[q] = jnp.where(upper, x[q], pltpu.roll(x[p], LANES - TILE_S * m, 1))
                x = y
                m *= 2
            for p in range(pairs):
                tiles[b * pairs + p] = take_lanes(x[p], index)
            return carry

        lax.fori_loop(0, blocks, one, 0)

    @pl.when((step >= pairs) & (step < pairs + steps))
    def _():
        def one(i, carry):
            fill((step - pairs) * PACK + i * STEP)
            rows_out = pl.ds(pl.multiple_of(i * STEP, 8), STEP)
            for j, shift in enumerate(shifts[skipped:]):
                outs[j][rows_out, :] = block_for(lax.rem(pos[0] + shift, peers))
            return carry

        lax.fori_loop(0, PACK // STEP, one, 0)

    @pl.when(step == pairs + steps)
    def _():
        fill(virtuals - LAST)

        def one(owner, carry):
            ends[owner] = block_for(owner)
            return carry

        lax.fori_loop(0, peers, one, 0)


def rest_blocks(shifts, peers, skipped, pos, order, half, v_high, v_low):
    pairs, basis, columns = half.shape
    virtuals = v_high.shape[0]
    n = len(shifts) - skipped
    cut = virtuals - LAST
    steps = cut // PACK
    results = pl.pallas_call(
        functools.partial(rest_kernel, shifts, peers, skipped),
        grid=(pairs + steps + 1,),
        in_specs=[
            SMEM,
            SMEM,
            pl.BlockSpec((1, basis, columns), lambda i: (jnp.minimum(i, pairs - 1), 0, 0)),
        ]
        + [pl.BlockSpec((virtuals, basis), lambda i: (0, 0))] * 2,
        out_specs=[pl.BlockSpec((PACK, LANES), lambda i: (jnp.clip(i - pairs, 0, steps - 1), 0))] * n
        + [
            pl.BlockSpec((peers, LAST, LANES), lambda i: (0, 0, 0)),
            pl.BlockSpec((1, 8, LANES), lambda i: (jnp.minimum(i, pairs - 1), 0, 0)),
        ],
        out_shape=[jax.ShapeDtypeStruct((cut, LANES), jnp.float32)] * n
        + [
            jax.ShapeDtypeStruct((peers, LAST, LANES), jnp.float32),
            jax.ShapeDtypeStruct((pairs, 8, LANES), jnp.float32),
        ],
        scratch_shapes=[
            pltpu.VMEM((pairs, virtuals, columns), jnp.float32),
            pltpu.VMEM((columns * pairs // LANES, STEP, LANES), jnp.float32),
        ],
        cost_estimate=pl.CostEstimate(
            flops=6 * pairs * columns * basis * virtuals,
            bytes_accessed=4 * pairs * basis * columns,
            transcendentals=0,
        ),
        name="rest_blocks",
    )(pos, order, half, v_high, v_low)
    return results[:n], results[n], results[n + 1]


def merge(x, pairs, ahead):
    n = len(x)
    group = lax.broadcasted_iota(jnp.int32, x[0].shape, 1) // pairs
    behind = (group - ahead + n) % n
    m = 1
    while m < n:
        far = (behind & m) != 0
        x = [jnp.where(far, x[(j + m) % n], x[j]) for j in range(n)]
        m *= 2
    turns = [(LANES - k * pairs) % LANES for k in range(n)]
    return [pltpu.roll(x[-k % n], t, 1) if t else x[0] for k, t in enumerate(turns)]


def unpack_kernel(peers, pairs, pos, weights, *refs):
    ins, out = refs[:peers], refs[-1]
    per = LANES // pairs
    ahead = lax.rem(pos[0], per)
    outer = lax.div(pos[0], per)
    group = lax.broadcasted_iota(jnp.int32, (8, LANES), 1) // pairs
    straight = group >= ahead
    count = peers // per

    def one(step, carry):
        for t in range(UNROLL):
            rows = pl.ds(pl.multiple_of((step * UNROLL + t) * 8, 8), 8)
            halves = [
                merge([ins[b * per + j][rows, :] for j in range(per)], pairs, ahead)
                for b in range(count)
            ]
            for b in range(count):
                place = pl.multiple_of(lax.rem(b + outer, count) * LANES, LANES)
                scale = weights[:, pl.ds(place, LANES)]
                for k in range(per):
                    value = jnp.where(straight, halves[b][k], halves[b - 1][k])
                    out[k, rows, pl.ds(place, LANES)] = value * scale
        return carry

    lax.fori_loop(0, out.shape[1] // (8 * UNROLL), one, 0)


def unpack(blocks, pos, weights, pairs, virtuals):
    peers = len(blocks)
    per = LANES // pairs
    total = weights.shape[1]
    return pl.pallas_call(
        functools.partial(unpack_kernel, peers, pairs),
        grid=(blocks[0].shape[0] // UNPACK,),
        in_specs=[SMEM, pl.BlockSpec((1, total), lambda i: (0, 0))]
        + [pl.BlockSpec((UNPACK, LANES), lambda i: (i, 0))] * peers,
        out_specs=pl.BlockSpec((per, UNPACK, total), lambda i: (0, i, 0)),
        out_shape=jax.ShapeDtypeStruct((per, virtuals, total), jnp.float32),
        compiler_params=pltpu.CompilerParams(vmem_limit_bytes=UNPACK_VMEM),
        name="unpack",
    )(pos, weights, *blocks)


def unpack_last_kernel(pairs, weights, ends, _, out):
    peers, rows, _ = ends.shape
    per = LANES // pairs

    def one(step, carry):
        at = pl.ds(pl.multiple_of(step * 8, 8), 8)
        for b in range(peers // per):
            lanes = pl.ds(b * LANES, LANES)
            done = merge([ends[b * per + j, at, :] for j in range(per)], pairs, 0)
            for k in range(per):
                out[k, at, lanes] = done[k] * weights[:, lanes]
        return carry

    lax.fori_loop(0, rows // 8, one, 0, unroll=True)


def unpack_last(ends, weights, pairs, into):
    per, virtuals, total = into.shape
    rows = ends.shape[1]
    return pl.pallas_call(
        functools.partial(unpack_last_kernel, pairs),
        grid=(1,),
        in_specs=[
            pl.BlockSpec((1, total), lambda i: (0, 0)),
            pl.BlockSpec(ends.shape, lambda i: (0, 0, 0)),
            ANY,
        ],
        out_specs=pl.BlockSpec((per, rows, total), lambda i: (0, virtuals // rows - 1, 0)),
        out_shape=jax.ShapeDtypeStruct(into.shape, into.dtype),
        input_output_aliases={2: 0},
        name="unpack_last",
    )(weights, ends, into)


def order_of_shifts(peers):
    middle = peers // 4
    distances = [middle] + [d for d in range(peers // 2 - 1, 0, -1) if d != middle]
    shifts = []
    for d in distances:
        shifts += [d, peers - d]
    shifts.insert(sum(EARLY), peers // 2)
    return shifts + [0]


def shards(half_integrals, pair_list, occupied_energy, virtual_orbitals, tile_order):
    pairs, columns, _ = half_integrals.shape
    virtuals = virtual_orbitals.shape[1]
    peers = lax.axis_size("wide")
    cut = virtuals - LAST
    pos = lax.axis_index("wide").astype(jnp.int32).reshape(1)
    half = jnp.swapaxes(half_integrals, 1, 2)
    shifts = tuple(order_of_shifts(peers))
    blocks = []
    kept = [virtual_orbitals]
    at = 0
    for n in EARLY:
        results = early_blocks(shifts[at : at + n], peers, cut, pos, tile_order, half, *kept)
        blocks += results[:n]
        kept = results[n:] or kept
        at += n
    more, ends, sums = rest_blocks(shifts, peers, at, pos, tile_order, half, *kept)
    blocks += more
    arrived = {}
    for n, s in enumerate(shifts):
        block = blocks[n]
        if s:
            block = lax.ppermute(block, "wide", [(i, (i + s) % peers) for i in range(peers)])
        arrived[(peers - s) % peers] = block
    squares = jnp.sum(sums, axis=(1, 2))
    sent = jnp.broadcast_to(squares[None, None], (peers, 1, pairs))
    totals = lax.all_to_all(sent, "wide", 0, 0, tiled=True).reshape(peers * pairs)
    ends = lax.all_to_all(ends, "wide", 0, 0, tiled=True)
    weights = pair_weights(pair_list, occupied_energy)
    pair_rms = jnp.sqrt(totals * weights * weights / (columns * virtuals) + 1e-06)
    out = unpack([arrived[i] for i in range(peers)], pos, weights[None], pairs, virtuals)
    out = unpack_last(ends, weights[None], pairs, out)
    return (jnp.transpose(out, (2, 0, 1)), pair_rms)


def solution(mesh):
    in_specs = (
        P(("groups", "wide"), None, None),
        P("groups", None),
        P("groups"),
        P("groups", None),
        P(),
    )
    out_specs = (P("groups", "wide", None), P("groups"))
    return jax.shard_map(shards, mesh=mesh, in_specs=in_specs, out_specs=out_specs, check_vma=False)
```
